32 devices in a mesh: rows: 8 (over y, x, core), cols: 4 (over z).
Axes of the slice: x: 2, y: 2, z: 4, core: 2. Of those that a mesh axis runs over, the one named last changes fastest.
Arguments:
- coarse: float32 [512, 512], P('rows', 'cols'), may hold values from -6 to 6
- detail4: float32 [3, 512, 512], P(None, 'rows', 'cols'), may hold values from -6 to 6
- detail3: float32 [3, 1024, 1024], P(None, 'rows', 'cols'), may hold values from -6 to 6
- detail2: float32 [3, 2048, 2048], P(None, 'rows', 'cols'), may hold values from -6 to 6
- detail1: float32 [3, 4096, 4096], P(None, 'rows', 'cols'), may hold values from -6 to 6
Outputs:
- image: float32 [8192, 8192], P('rows', 'cols')
The draws below stay inside these ranges and needn't reach their ends.
All inputs are finite; a program needn't handle non-finite values.
Results may differ from the reference program's by a relative error of at most 0.00013.
Values sent between devices are 32-bit elements; how exact they have to be, the bound alone decides.
A program may use at most 128 MiB of HBM per device.

```python
import jax
import jax.numpy as jnp

NR = 8192
NC = 8192


def steps_of(rng, dims, shards, smallest, high):
    def one(position, blocks):
        draws = jax.random.uniform(jax.random.fold_in(jax.random.fold_in(rng, 6), position), (blocks,), jnp.float32, smallest / len(shards), high / len(shards))
        return jnp.repeat(jnp.exp(draws), dims[position] // blocks).reshape((-1,) + (1,) * (len(dims) - position - 1))

    loudness = one(*shards[0])
    for cut in shards[1:]:
        loudness = loudness * one(*cut)
    return loudness


def noise(own_key, extent, deviation, reach, cuts=(), kind=jnp.bfloat16):
    result = deviation * jax.random.normal(own_key, extent, jnp.float32)
    if cuts:
        result = result * steps_of(own_key, extent, cuts, -0.22, 0.18)
    return jnp.clip(result, -reach, reach).astype(kind)


def setup_inputs(seed: int = 0) -> dict:
    splits = jax.random.split(jax.random.key(seed), 6)
    coarse = noise(splits[0], (NR // 16, NC // 16), 1.0, 6.0, ((0, 8), (1, 4)), jnp.float32)
    detail4 = noise(splits[1], (3, NR // 16, NC // 16), 1.0, 6.0, ((1, 8), (2, 4)), jnp.float32)
    detail3 = noise(splits[2], (3, NR // 8, NC // 8), 1.0, 6.0, ((1, 8), (2, 4)), jnp.float32)
    detail2 = noise(splits[3], (3, NR // 4, NC // 4), 1.0, 6.0, ((1, 8), (2, 4)), jnp.float32)
    detail1 = noise(splits[4], (3, NR // 2, NC // 2), 1.0, 6.0, ((1, 8), (2, 4)), jnp.float32)
    return {"coarse": coarse, "detail4": detail4, "detail3": detail3, "detail2": detail2, "detail1": detail1}


lift_alpha = -1.586134342059924
lift_beta = -0.052980118572961
lift_gamma = 0.882911075530934
lift_delta = 0.443506852043971
lift_scale = 1.149604398860241


def phase_join(smooth, rough, along):
    target = list(smooth.shape)
    target[along] = 2 * target[along]
    return jnp.stack((smooth, rough), axis=along + 1).reshape(target)


def lift_roll(smooth, rough, along):
    smooth = smooth * lift_scale
    rough = rough / lift_scale
    smooth = smooth - lift_delta * (rough + jnp.roll(rough, 1, along))
    rough = rough - lift_gamma * (smooth + jnp.roll(smooth, -1, along))
    smooth = smooth - lift_beta * (rough + jnp.roll(rough, 1, along))
    rough = rough - lift_alpha * (smooth + jnp.roll(smooth, -1, along))
    return phase_join(smooth, rough, along)


def whole_synth(lowband, detail):
    smooth = jnp.stack((lowband, detail[1]), 0)
    rough = jnp.stack((detail[0], detail[2]), 0)
    halves = lift_roll(smooth, rough, 2)
    return lift_roll(halves[0], halves[1], 0)


def reference(coarse, detail4, detail3, detail2, detail1):
    lowband = coarse
    for detail in (detail4, detail3, detail2, detail1):
        lowband = whole_synth(lowband, detail)
    return lowband
```

```python
import functools

import jax
import jax.numpy as jnp
from jax import lax
from jax.experimental import pallas as pl
from jax.experimental.pallas import tpu as pltpu
from jax.sharding import PartitionSpec as P

lift_alpha = -1.586134342059924
lift_beta = -0.052980118572961
lift_gamma = 0.882911075530934
lift_delta = 0.443506852043971
lift_scale = 1.149604398860241

MESH = pl.DeviceIdType.MESH
LANES = 128
SUB = 8
BIG, SMALL = lift_scale * lift_scale, 1.0 / (lift_scale * lift_scale)


def lanes_of(shape):
    return lax.broadcasted_iota(jnp.int32, shape, len(shape) - 1)


def rows_of(shape):
    return lax.broadcasted_iota(jnp.int32, shape, len(shape) - 2)


def eight(start):
    return pl.ds(pl.multiple_of(start, SUB), SUB)


def block(start):
    return pl.ds(pl.multiple_of(start, SUB), LANES)


def lift(get_smooth, get_rough, put_even, put_odd, steps):
    before = get_rough(-1)
    smooth = get_smooth(-1) - lift_delta * (before + get_rough(-2))
    r0 = get_rough(0)
    s1 = get_smooth(0) - lift_delta * (r0 + before)
    r2_before = before - lift_gamma * (smooth + s1)
    r0_next = get_rough(1)
    s1_next = get_smooth(1) - lift_delta * (r0_next + r0)
    r2 = r0 - lift_gamma * (s1 + s1_next)
    s3 = s1 - lift_beta * (r2 + r2_before)
    s1, r0 = s1_next, r0_next
    for v in range(steps):
        r0_next = get_rough(v + 2)
        s1_next = get_smooth(v + 2) - lift_delta * (r0_next + r0)
        r2_next = r0 - lift_gamma * (s1 + s1_next)
        s3_next = s1 - lift_beta * (r2_next + r2)
        put_even(v, s3)
        put_odd(v, r2 - lift_alpha * (s3 + s3_next))
        s1, r0, r2, s3 = s1_next, r0_next, r2_next, s3_next


def vertical(smooth_ref, rough_ref, out_ref, height, half):
    steps = (height + SUB) // SUB

    def smooth(v):
        x = smooth_ref[pl.ds(4 + v, SUB, stride=steps), :]
        return x * BIG if half == 0 else x

    def rough(v):
        x = rough_ref[pl.ds(4 + v, SUB, stride=steps), :]
        return x * SMALL if half == 1 else x

    def even(v, x):
        out_ref[pl.ds(2 * v, SUB, stride=2 * steps), :] = x

    def odd(v, x):
        out_ref[pl.ds(2 * v + 1, SUB, stride=2 * steps), :] = x

    lift(smooth, rough, even, odd, steps)


def horizontal(turned, spread, width, wrap):
    steps = (width + SUB) // SUB

    def smooth(v):
        return turned[0, pl.ds(4 + v, SUB, stride=steps), :]

    def rough(v):
        return turned[1, pl.ds(4 + v, SUB, stride=steps), :]

    def even(v, x):
        spread[pl.ds(2 * v, SUB, stride=2 * steps), :] = x

    def odd(v, x):
        spread[pl.ds(2 * v + 1, SUB, stride=2 * steps), :] = x

    lift(smooth, rough, even, odd, steps)
    if wrap:
        spread[pl.ds(SUB + 2 * width + LANES - SUB, SUB), :] = spread[pl.ds(0, SUB), :]


def turn_in(joined, turned, k, tiles):
    for half in range(2):
        for c in range(tiles + 1):
            turned[half, pl.ds(SUB + LANES * c, LANES), :] = joined[
                half, c, block(SUB + LANES * k), :
            ].T
        turned[half, pl.ds(0, SUB), :] = turned[
            half, pl.ds(SUB + LANES * tiles + LANES - SUB, SUB), :
        ]


def blocks_of(count, tin, across, tout, turned, spread):
    tin(0, turned[0])
    across(turned[0], spread[0])
    if count > 1:
        tin(1, turned[1])
    pairs = (count - 1) // 2

    def two(m, carry):
        k = 2 * m
        tout(k, spread[0])
        across(turned[1], spread[1])
        tin(k + 2, turned[0])
        tout(k + 1, spread[1])
        across(turned[0], spread[0])
        tin(jnp.minimum(k + 3, count - 1), turned[1])
        return carry

    if pairs:
        lax.fori_loop(0, pairs, two, 0)
    if count % 2:
        tout(count - 1, spread[0])
    else:
        tout(count - 2, spread[0])
        across(turned[1], spread[1])
        tout(count - 1, spread[1])


def row_items(levels):
    return [(a, b, c) for a, (n, h, w) in enumerate(levels) for b in range(n) for c in range(w // LANES)]


def column_blocks(levels):
    blocks, short = [], []
    for a, (n, h, w) in enumerate(levels):
        for b in range(n):
            if h < LANES:
                short.append((a, b, 0, h))
                if sum(p[3] for p in short) == LANES:
                    blocks.append(short)
                    short = []
            else:
                blocks.extend([[(a, b, LANES * k, LANES)] for k in range(h // LANES)])
    return blocks + ([short] if short else [])


def coarse_levels(mesh_shape, levels, *refs):
    count = len(levels)
    inputs, refs = refs[:count], refs[count:]
    low_out, detail_out, refs = refs[0], refs[1], refs[2:]
    lows, refs = list(refs[: count - 2]) + [low_out], refs[count - 2 :]
    details, refs = list(refs[: count - 2]) + [detail_out], refs[count - 2 :]
    tops, bottoms, refs = refs[:count], refs[count : 2 * count], refs[2 * count :]
    joined, turned_a, turned_b, spread_a, spread_b, *refs = refs
    send_top, send_bottom, below, above, *refs = refs
    send_first, send_last, from_right, from_left, *refs = refs
    corner_top, corner_bottom, down_right, down_left, up_right, up_left, *refs = refs
    edge_sem, body_sem, send_sem, recv_sem = refs

    def band(a, b):
        return lows[0] if a == 0 else details[a - 1].at[b]

    n_rows, n_cols = mesh_shape
    row, col = lax.axis_index("rows"), lax.axis_index("cols")
    row_next, row_prev = lax.rem(row + 1, n_rows), lax.rem(row + n_rows - 1, n_rows)
    col_next, col_prev = lax.rem(col + 1, n_cols), lax.rem(col + n_cols - 1, n_cols)

    barrier = pltpu.get_barrier_semaphore()
    neighbours = [
        (r, c)
        for r in (row_prev, row, row_next)
        for c in (col_prev, col, col_next)
        if not (r is row and c is col)
    ]
    for place in neighbours:
        pl.semaphore_signal(barrier, inc=1, device_id=place, device_id_type=MESH)

    edges, bodies = [], []

    def load(src, dst, sem, into):
        copy = pltpu.make_async_copy(src, dst, sem.at[len(into)])
        copy.start()
        into.append(copy)

    def load_tile(a, c, sem, into):
        n, h, w = levels[a]
        src = inputs[a].at[:, :, pl.ds(c * LANES, LANES)]
        if a == 0:
            dst = lows[0].at[pl.ds(c, 1), pl.ds(SUB, h), :]
        else:
            dst = details[a - 1].at[:, c, pl.ds(SUB, h), :]
        load(src, dst, sem, into)

    for a in reversed(range(count)):
        n, h, w = levels[a]
        load(inputs[a].at[:, pl.ds(0, SUB), :], tops[a], edge_sem, edges)
        load(inputs[a].at[:, pl.ds(h - SUB, SUB), :], bottoms[a], edge_sem, edges)
        for c in sorted({0, w // LANES - 1}):
            load_tile(a, c, edge_sem, edges)
    for a in range(count):
        for c in range(1, levels[a][2] // LANES - 1):
            load_tile(a, c, body_sem, bodies)

    lane = lanes_of((SUB, LANES))
    sub = rows_of((SUB, LANES))
    upper = sub < 4

    for copy in edges:
        copy.wait()

    items = row_items(levels)
    for k in range((len(items) + 1) // 2):
        pair = items[2 * k : 2 * k + 2]
        top, bottom = [
            [ref[a][b, :, pl.ds(c * LANES, LANES)] for a, b, c in pair] for ref in (tops, bottoms)
        ]
        top, bottom = [x if len(x) == 2 else x * 2 for x in (top, bottom)]
        send_top[k] = jnp.where(upper, top[0], pltpu.roll(top[1], 4, 0))
        send_bottom[k] = jnp.where(upper, pltpu.roll(bottom[1], 4, 0), bottom[0])

    corner_items = [(a, b) for a in range(count) for b in range(levels[a][0])]
    slot = lax.rem(lane + 4, LANES) // 8
    for ref, out in ((tops, corner_top), (bottoms, corner_bottom)):
        total = None
        for p, (a, b) in enumerate(corner_items):
            w = levels[a][2]
            edge = jnp.where(
                lane < 64, ref[a][b, :, pl.ds(0, LANES)], ref[a][b, :, pl.ds(w - LANES, LANES)]
            )
            if p:
                edge = pltpu.roll(edge, 8 * p, 1)
            total = edge if total is None else jnp.where(slot == p, edge, total)
        out[...] = total

    pl.semaphore_wait(barrier, len(neighbours))

    sends = []

    def send(src, dst, place):
        k = len(sends)
        copy = pltpu.make_async_remote_copy(
            src_ref=src,
            dst_ref=dst,
            send_sem=send_sem.at[k],
            recv_sem=recv_sem.at[k],
            device_id=place,
            device_id_type=MESH,
        )
        copy.start()
        sends.append(copy)

    send(send_top, below, (row_prev, col))
    send(send_bottom, above, (row_next, col))
    send(corner_top, down_right, (row_prev, col_prev))
    send(corner_top, down_left, (row_prev, col_next))
    send(corner_bottom, up_right, (row_next, col_prev))
    send(corner_bottom, up_left, (row_next, col_next))

    blocks = column_blocks(levels)
    first_half = lanes_of((LANES, LANES)) < 64
    turned = []
    for parts in blocks:
        pieces = []
        for a, b, start, length in parts:
            w = levels[a][2]
            rows = pl.ds(SUB + start, length)
            pieces.append(
                jnp.where(
                    first_half[:length],
                    band(a, b)[0, rows, :],
                    band(a, b)[w // LANES - 1, rows, :],
                )
            )
        missing = LANES - sum(p[3] for p in parts)
        if missing:
            pieces.append(jnp.zeros((missing, LANES), jnp.float32))
        whole = pieces[0] if len(pieces) == 1 else jnp.concatenate(pieces, axis=0)
        whole = whole.T
        turned.append((whole[:SUB], whole[LANES - SUB :]))
    for k in range((len(blocks) + 1) // 2):
        one = turned[2 * k]
        two = turned[min(2 * k + 1, len(blocks) - 1)]
        send_first[k] = jnp.where(upper, one[0], pltpu.roll(two[0], 4, 0))
        send_last[k] = jnp.where(upper, pltpu.roll(two[1], 4, 0), one[1])
    send(send_first, from_right, (row, col_prev))
    send(send_last, from_left, (row, col_next))

    for copy in bodies:
        copy.wait()
    for copy in sends:
        copy.wait()

    for k in range((len(items) + 1) // 2):
        for i, (a, b, c) in enumerate(items[2 * k : 2 * k + 2]):
            h = levels[a][1]
            after, before = below[k], above[k]
            if i:
                after, before = pltpu.roll(after, 4, 0), pltpu.roll(before, 4, 0)
            band(a, b)[c, pl.ds(SUB + h, SUB), :] = after
            band(a, b)[c, pl.ds(0, SUB), :] = before
    for k in range((len(blocks) + 1) // 2):
        for i, parts in enumerate(blocks[2 * k : 2 * k + 2]):
            after, before = from_right[k], from_left[k]
            if i:
                after, before = pltpu.roll(after, 4, 0), pltpu.roll(before, 4, 0)
            whole = jnp.concatenate(
                [after, jnp.zeros((LANES - 2 * SUB, LANES), jnp.float32), before], axis=0
            ).T
            place = 0
            for a, b, start, length in parts:
                band(a, b)[levels[a][2] // LANES, pl.ds(SUB + start, length), :] = whole[
                    place : place + length
                ]
                place += length
    right_side = lax.rem(lane, 8) < 4
    corner = jnp.where(
        upper,
        jnp.where(right_side, down_right[...], down_left[...]),
        jnp.where(right_side, up_right[...], up_left[...]),
    )
    for p, (a, b) in enumerate(corner_items):
        n, h, w = levels[a]
        here = pltpu.roll(corner, LANES - 8 * p, 1) if p else corner
        band(a, b)[w // LANES, pl.ds(0, SUB), :] = here
        band(a, b)[w // LANES, pl.ds(SUB + h, SUB), :] = here

    for level in range(count - 2):
        n, h, w = levels[level + 1]
        tiles = w // LANES
        low, detail, target = lows[level], details[level], lows[level + 1]

        def columns(c, carry):
            for half in range(2):
                smooth = low.at[c] if half == 0 else detail.at[0, c]
                rough = detail.at[1, c] if half == 0 else detail.at[2, c]
                out = joined.at[half, c]
                vertical(smooth, rough, out, h, half)
                out[pl.ds(SUB + 2 * h + LANES - SUB, SUB), :] = out[pl.ds(0, SUB), :]
            return carry

        lax.fori_loop(0, tiles + 1, columns, 0)

        def tin(k, turned):
            turn_in(joined, turned, k, tiles)

        def across(turned, spread):
            horizontal(turned, spread, w, True)

        def tout(k, spread):
            for j in range(2 * tiles + 1):
                target[j, block(SUB + LANES * k), :] = spread[pl.ds(SUB + LANES * j, LANES), :].T

        blocks_of(2 * h // LANES + 1, tin, across, tout, (turned_a, turned_b), (spread_a, spread_b))
        for j in range(2 * tiles + 1):
            target[j, pl.ds(0, SUB), :] = target[j, pl.ds(SUB + 2 * h + LANES - SUB, SUB), :]


def finest_level(height, width, low, detail, out, joined, *refs):
    turned_a, turned_b, spread_a, spread_b, finished, store_sem = refs
    tiles = width // LANES

    def columns(c, carry):
        for half in range(2):
            smooth = low.at[c] if half == 0 else detail.at[0, c]
            rough = detail.at[1, c] if half == 0 else detail.at[2, c]
            vertical(smooth, rough, joined.at[half, c], height, half)
        return carry

    lax.fori_loop(0, tiles + 1, columns, 0)

    def store_copy(k, j):
        rows = block(LANES * k)
        return pltpu.make_async_copy(
            finished.at[j, rows, :], out.at[rows, pl.ds(j * LANES, LANES)], store_sem.at[k, j]
        )

    def tin(k, turned):
        turn_in(joined, turned, k, tiles)

    def across(turned, spread):
        horizontal(turned, spread, width, False)

    def tout(k, spread):
        for j in range(2 * tiles):
            finished[j, block(LANES * k), :] = spread[pl.ds(SUB + LANES * j, LANES), :].T
            store_copy(k, j).start()

    count = 2 * height // LANES
    blocks_of(count, tin, across, tout, (turned_a, turned_b), (spread_a, spread_b))
    for k in range(count):
        for j in range(2 * tiles):
            store_copy(k, j).wait()


def per_device(mesh_shape, coarse, *details):
    arrays = (coarse[None],) + details
    arrays = tuple(pltpu.with_memory_space_constraint(a, pltpu.HBM) for a in arrays)
    levels = [a.shape for a in arrays]
    count = len(levels)
    f32 = jnp.float32
    vmem = lambda *dims: pltpu.VMEM(dims, f32)
    anywhere = pl.BlockSpec(memory_space=pl.ANY)
    in_vmem = pl.BlockSpec(memory_space=pltpu.VMEM)
    n_pairs = (len(row_items(levels)) + 1) // 2
    n_blocks = (len(column_blocks(levels)) + 1) // 2
    n_edges = sum(2 + len({0, w // LANES - 1}) for n, h, w in levels)
    n_bodies = sum(max(w // LANES - 2, 0) for n, h, w in levels)
    n, h, w = levels[-2]
    low_shape = lambda h, w: (w // LANES + 1, SUB + h + LANES, LANES)
    detail_shape = lambda h, w: (3, w // LANES + 1, h + 2 * SUB, LANES)
    _, height, width = levels[-1]
    low, detail = pl.pallas_call(
        functools.partial(coarse_levels, mesh_shape, levels),
        out_shape=[vmem(*low_shape(height, width)), vmem(*detail_shape(height, width))],
        in_specs=[anywhere] * count,
        out_specs=[in_vmem] * 2,
        scratch_shapes=[vmem(*low_shape(h, w)) for _, h, w in levels[1:-1]]
        + [vmem(*detail_shape(h, w)) for _, h, w in levels[1:-1]]
        + [vmem(b, SUB, w) for b, h, w in levels] * 2
        + [vmem(2, w // LANES + 1, SUB + 2 * h + LANES, LANES)]
        + [vmem(2, SUB + w + LANES, LANES)] * 2
        + [vmem(SUB + 2 * w + LANES, LANES)] * 2
        + [vmem(n_pairs, SUB, LANES)] * 4
        + [vmem(n_blocks, SUB, LANES)] * 4
        + [vmem(SUB, LANES)] * 6
        + [
            pltpu.SemaphoreType.DMA((n_edges,)),
            pltpu.SemaphoreType.DMA((max(n_bodies, 1),)),
            pltpu.SemaphoreType.DMA((8,)),
            pltpu.SemaphoreType.DMA((8,)),
        ],
        compiler_params=pltpu.CompilerParams(
            collective_id=0, has_side_effects=True, vmem_limit_bytes=40 * 1024 * 1024
        ),
        name="coarse_levels",
    )(*arrays)

    tiles = width // LANES
    return pl.pallas_call(
        functools.partial(finest_level, height, width),
        out_shape=jax.ShapeDtypeStruct((2 * height, 2 * width), f32),
        in_specs=[in_vmem] * 2,
        out_specs=anywhere,
        scratch_shapes=[vmem(2, tiles + 1, 2 * height + 2 * SUB, LANES)]
        + [vmem(2, SUB + width + LANES, LANES)] * 2
        + [vmem(2 * width + 2 * SUB, LANES)] * 2
        + [
            vmem(2 * tiles, 2 * height, LANES),
            pltpu.SemaphoreType.DMA((2 * height // LANES, 2 * tiles)),
        ],
        compiler_params=pltpu.CompilerParams(vmem_limit_bytes=40 * 1024 * 1024),
        name="finest_level",
    )(low, detail)


def solution(mesh):
    mesh_shape = (mesh.shape["rows"], mesh.shape["cols"])
    return jax.shard_map(
        functools.partial(per_device, mesh_shape),
        mesh=mesh,
        in_specs=(
            P("rows", "cols"),
            P(None, "rows", "cols"),
            P(None, "rows", "cols"),
            P(None, "rows", "cols"),
            P(None, "rows", "cols"),
        ),
        out_specs=P("rows", "cols"),
        check_vma=False,
    )
```

```python
import functools

import jax
import jax.numpy as jnp
from jax import lax
from jax.experimental import pallas as pl
from jax.experimental.pallas import tpu as pltpu
from jax.sharding import PartitionSpec as P

lift_alpha = -1.586134342059924
lift_beta = -0.052980118572961
lift_gamma = 0.882911075530934
lift_delta = 0.443506852043971
lift_scale = 1.149604398860241

MESH = pl.DeviceIdType.MESH
LANES = 128
SUB = 8
STRIP = 72
BIG, SMALL = lift_scale * lift_scale, 1.0 / (lift_scale * lift_scale)


def lanes_of(shape):
    return lax.broadcasted_iota(jnp.int32, shape, len(shape) - 1)


def rows_of(shape):
    return lax.broadcasted_iota(jnp.int32, shape, len(shape) - 2)


def eight(start):
    return pl.ds(pl.multiple_of(start, SUB), SUB)


def block(start):
    return pl.ds(pl.multiple_of(start, SUB), LANES)


def lift(get_smooth, get_rough, put_even, put_odd, steps):
    before = get_rough(-1)
    smooth = get_smooth(-1) - lift_delta * (before + get_rough(-2))
    r0 = get_rough(0)
    s1 = get_smooth(0) - lift_delta * (r0 + before)
    r2_before = before - lift_gamma * (smooth + s1)
    r0_next = get_rough(1)
    s1_next = get_smooth(1) - lift_delta * (r0_next + r0)
    r2 = r0 - lift_gamma * (s1 + s1_next)
    s3 = s1 - lift_beta * (r2 + r2_before)
    s1, r0 = s1_next, r0_next
    for v in range(steps):
        r0_next = get_rough(v + 2)
        s1_next = get_smooth(v + 2) - lift_delta * (r0_next + r0)
        r2_next = r0 - lift_gamma * (s1 + s1_next)
        s3_next = s1 - lift_beta * (r2_next + r2)
        put_even(v, s3)
        put_odd(v, r2 - lift_alpha * (s3 + s3_next))
        s1, r0, r2, s3 = s1_next, r0_next, r2_next, s3_next


def vertical(smooth_ref, rough_ref, out_ref, steps, half, first=4):
    def smooth(v):
        x = smooth_ref[pl.ds(first + v, SUB, stride=steps), :]
        return x * BIG if half == 0 else x

    def rough(v):
        x = rough_ref[pl.ds(first + v, SUB, stride=steps), :]
        return x * SMALL if half == 1 else x

    def even(v, x):
        out_ref[pl.ds(2 * v, SUB, stride=2 * steps), :] = x

    def odd(v, x):
        out_ref[pl.ds(2 * v + 1, SUB, stride=2 * steps), :] = x

    lift(smooth, rough, even, odd, steps)


def horizontal(smooth_ref, rough_ref, spread, width, wrap):
    steps = (width + SUB) // SUB

    def smooth(v):
        return smooth_ref[pl.ds(4 + v, SUB, stride=steps), :]

    def rough(v):
        return rough_ref[pl.ds(4 + v, SUB, stride=steps), :]

    def even(v, x):
        spread[pl.ds(2 * v, SUB, stride=2 * steps), :] = x

    def odd(v, x):
        spread[pl.ds(2 * v + 1, SUB, stride=2 * steps), :] = x

    lift(smooth, rough, even, odd, steps)
    if wrap:
        spread[pl.ds(SUB + 2 * width + LANES - SUB, SUB), :] = spread[pl.ds(0, SUB), :]


def turn_in(joined, turned, k, tiles):
    for c in range(tiles + 1):
        turned[pl.ds(SUB + LANES * c, LANES), :] = joined[c, block(SUB + LANES * k), :].T
    wrap_around(turned, tiles)


def wrap_around(turned, tiles):
    turned[pl.ds(0, SUB), :] = turned[pl.ds(SUB + LANES * tiles + LANES - SUB, SUB), :]


def blocks_of(count, tin, across, tout):
    tin(0, 0)
    across(0, 0)
    if count > 1:
        tin(1, 1)
    pairs = (count - 1) // 2

    def two(m, carry):
        k = 2 * m
        tout(k, 0)
        across(k + 1, 1)
        tin(k + 2, 0)
        tout(k + 1, 1)
        across(k + 2, 0)
        tin(jnp.minimum(k + 3, count - 1), 1)
        return carry

    if pairs:
        lax.fori_loop(0, pairs, two, 0)
    if count % 2:
        tout(count - 1, 0)
    else:
        tout(count - 2, 0)
        across(count - 1, 1)
        tout(count - 1, 1)


def row_split(levels):
    return (len(row_items(levels[:-1])) + 1) // 2


def column_split(levels):
    return (len(column_blocks(levels[:-1])) + 1) // 2


def row_items(levels):
    return [(a, b, c) for a, (n, h, w) in enumerate(levels) for b in range(n) for c in range(w // LANES)]


def column_blocks(levels):
    blocks, short = [], []
    for a, (n, h, w) in enumerate(levels):
        for b in range(n):
            if h < LANES:
                short.append((a, b, 0, h))
                if sum(p[3] for p in short) == LANES:
                    blocks.append(short)
                    short = []
            else:
                blocks.extend([[(a, b, LANES * k, LANES)] for k in range(h // LANES)])
    return blocks + ([short] if short else [])


def coarse_levels(mesh_shape, levels, *refs):
    count = len(levels)
    inputs, refs = refs[:count], refs[count:]
    low_out, mixed_out, rough_out, refs = refs[0], refs[1], refs[2], refs[3:]
    lows, refs = list(refs[: count - 2]) + [low_out], refs[count - 2 :]
    details, refs = refs[: count - 2], refs[count - 2 :]
    outer, refs = refs[0], refs[1:]
    tops, bottoms, refs = refs[:count], refs[count : 2 * count], refs[2 * count :]
    joined, smooth_a, smooth_b, rough_a, rough_b, spread_a, spread_b, *refs = refs
    strip, tall_a, tall_b, *refs = refs
    send_top, send_bottom, below, above, *refs = refs
    send_first, send_last, from_right, from_left, *refs = refs
    corner_top, corner_bottom, down_right, down_left, up_right, up_left, *refs = refs
    edge_sem, body_sem, send_sem, recv_sem = refs

    def band(a, b):
        if a == 0:
            return lows[0]
        if a < count - 1:
            return details[a - 1].at[b]
        return mixed_out if b == 1 else outer.at[b // 2]

    n_rows, n_cols = mesh_shape
    row, col = lax.axis_index("rows"), lax.axis_index("cols")
    row_next, row_prev = lax.rem(row + 1, n_rows), lax.rem(row + n_rows - 1, n_rows)
    col_next, col_prev = lax.rem(col + 1, n_cols), lax.rem(col + n_cols - 1, n_cols)

    barrier = pltpu.get_barrier_semaphore()
    neighbours = [
        (r, c)
        for r in (row_prev, row, row_next)
        for c in (col_prev, col, col_next)
        if not (r is row and c is col)
    ]
    for place in neighbours:
        pl.semaphore_signal(barrier, inc=1, device_id=place, device_id_type=MESH)

    edges, bodies = [], []

    def load(src, dst, sem, into):
        copy = pltpu.make_async_copy(src, dst, sem.at[len(into)])
        copy.start()
        into.append(copy)

    def load_tile(a, c, sem, into):
        n, h, w = levels[a]
        columns = pl.ds(c * LANES, LANES)
        rows = pl.ds(SUB, h)
        if a == 0:
            load(inputs[a].at[:, :, columns], lows[0].at[pl.ds(c, 1), rows, :], sem, into)
        elif a < count - 1:
            load(inputs[a].at[:, :, columns], details[a - 1].at[:, c, rows, :], sem, into)
        else:
            for b in range(n):
                load(inputs[a].at[b, :, columns], band(a, b).at[c, rows, :], sem, into)

    for a in reversed(range(count)):
        n, h, w = levels[a]
        load(inputs[a].at[:, pl.ds(0, SUB), :], tops[a], edge_sem, edges)
        load(inputs[a].at[:, pl.ds(h - SUB, SUB), :], bottoms[a], edge_sem, edges)
        for c in sorted({0, w // LANES - 1}):
            load_tile(a, c, edge_sem, edges)
    for a in range(count):
        for c in range(1, levels[a][2] // LANES - 1):
            load_tile(a, c, body_sem, bodies)

    lane = lanes_of((SUB, LANES))
    sub = rows_of((SUB, LANES))
    upper = sub < 4

    for copy in edges:
        copy.wait()

    items = row_items(levels)
    for k in range((len(items) + 1) // 2):
        pair = items[2 * k : 2 * k + 2]
        top, bottom = [
            [ref[a][b, :, pl.ds(c * LANES, LANES)] for a, b, c in pair] for ref in (tops, bottoms)
        ]
        top, bottom = [x if len(x) == 2 else x * 2 for x in (top, bottom)]
        send_top[k] = jnp.where(upper, top[0], pltpu.roll(top[1], 4, 0))
        send_bottom[k] = jnp.where(upper, pltpu.roll(bottom[1], 4, 0), bottom[0])

    corner_items = [(a, b) for a in range(count) for b in range(levels[a][0])]
    slot = lax.rem(lane + 4, LANES) // 8
    for ref, out in ((tops, corner_top), (bottoms, corner_bottom)):
        total = None
        for p, (a, b) in enumerate(corner_items):
            w = levels[a][2]
            edge = jnp.where(
                lane < 64, ref[a][b, :, pl.ds(0, LANES)], ref[a][b, :, pl.ds(w - LANES, LANES)]
            )
            if p:
                edge = pltpu.roll(edge, 8 * p, 1)
            total = edge if total is None else jnp.where(slot == p, edge, total)
        out[...] = total

    pl.semaphore_wait(barrier, len(neighbours))

    sends = []

    def send(src, dst, place):
        k = len(sends)
        copy = pltpu.make_async_remote_copy(
            src_ref=src,
            dst_ref=dst,
            send_sem=send_sem.at[k],
            recv_sem=recv_sem.at[k],
            device_id=place,
            device_id_type=MESH,
        )
        copy.start()
        sends.append(copy)

    few_pairs = row_split(levels)
    rest_pairs = (len(items) + 1) // 2 - few_pairs

    def send_rows(start, length):
        part = pl.ds(start, length)
        send(send_top.at[part], below.at[part], (row_prev, col))
        send(send_bottom.at[part], above.at[part], (row_next, col))

    send_rows(0, few_pairs)
    send(corner_top, down_right, (row_prev, col_prev))
    send(corner_top, down_left, (row_prev, col_next))
    send(corner_bottom, up_right, (row_next, col_prev))
    send(corner_bottom, up_left, (row_next, col_next))

    blocks = column_blocks(levels)
    first_half = lanes_of((LANES, LANES)) < 64
    turned = []
    for parts in blocks:
        pieces = []
        for a, b, start, length in parts:
            w = levels[a][2]
            rows = pl.ds(SUB + start, length)
            pieces.append(
                jnp.where(
                    first_half[:length],
                    band(a, b)[0, rows, :],
                    band(a, b)[w // LANES - 1, rows, :],
                )
            )
        missing = LANES - sum(p[3] for p in parts)
        if missing:
            pieces.append(jnp.zeros((missing, LANES), jnp.float32))
        whole = pieces[0] if len(pieces) == 1 else jnp.concatenate(pieces, axis=0)
        whole = whole.T
        turned.append((whole[:SUB], whole[LANES - SUB :]))
    for k in range((len(blocks) + 1) // 2):
        one = turned[2 * k]
        two = turned[min(2 * k + 1, len(blocks) - 1)]
        send_first[k] = jnp.where(upper, one[0], pltpu.roll(two[0], 4, 0))
        send_last[k] = jnp.where(upper, pltpu.roll(two[1], 4, 0), one[1])
    few_blocks = column_split(levels)
    rest_blocks = (len(blocks) + 1) // 2 - few_blocks

    def send_columns(start, length):
        part = pl.ds(start, length)
        send(send_first.at[part], from_right.at[part], (row, col_prev))
        send(send_last.at[part], from_left.at[part], (row, col_next))

    send_columns(0, few_blocks)
    early = len(sends)
    send_rows(few_pairs, rest_pairs)
    send_columns(few_blocks, rest_blocks)

    for copy in bodies:
        copy.wait()

    n, h, w = levels[-1]
    tiles = w // LANES
    steps = (h + SUB) // SUB
    last = 2 * h // LANES - 1

    def turn_tall(tall, c, ks):
        for k in ks:
            rough_out[k, block(SUB + LANES * c), :] = tall[block(SUB + LANES * k), :].T

    def turn_strips(c):
        for i, (k, first) in enumerate(((0, 0), (last, h + SUB - STRIP))):
            vertical(outer.at[0, c], outer.at[1, c], strip.at[i], STRIP // SUB, 1, 4 + first)
            rough_out[k, block(SUB + LANES * c), :] = strip[i, pl.ds(SUB, LANES), :].T

    inner = range(1, last)
    vertical(outer.at[0, 0], outer.at[1, 0], tall_a, steps, 1)

    def two_tiles(m, carry):
        c = 2 * m
        turn_tall(tall_a, c, inner)
        vertical(outer.at[0, c + 1], outer.at[1, c + 1], tall_b, steps, 1)
        after = jnp.minimum(c + 2, tiles - 1)
        turn_tall(tall_b, c + 1, inner)
        vertical(outer.at[0, after], outer.at[1, after], tall_a, steps, 1)
        return carry

    lax.fori_loop(0, tiles // 2, two_tiles, 0)

    def unpack_rows(k):
        for i, (a, b, c) in enumerate(items[2 * k : 2 * k + 2]):
            h = levels[a][1]
            after, before = below[k], above[k]
            if i:
                after, before = pltpu.roll(after, 4, 0), pltpu.roll(before, 4, 0)
            band(a, b)[c, pl.ds(SUB + h, SUB), :] = after
            band(a, b)[c, pl.ds(0, SUB), :] = before

    def unpack_columns(k):
        for i, parts in enumerate(blocks[2 * k : 2 * k + 2]):
            after, before = from_right[k], from_left[k]
            if i:
                after, before = pltpu.roll(after, 4, 0), pltpu.roll(before, 4, 0)
            whole = jnp.concatenate(
                [after, jnp.zeros((LANES - 2 * SUB, LANES), jnp.float32), before], axis=0
            ).T
            place = 0
            for a, b, start, length in parts:
                band(a, b)[levels[a][2] // LANES, pl.ds(SUB + start, length), :] = whole[
                    place : place + length
                ]
                place += length

    for copy in sends[:early]:
        copy.wait()
    for k in range(few_pairs):
        unpack_rows(k)
    for k in range(few_blocks):
        unpack_columns(k)
    right_side = lax.rem(lane, 8) < 4
    corner = jnp.where(
        upper,
        jnp.where(right_side, down_right[...], down_left[...]),
        jnp.where(right_side, up_right[...], up_left[...]),
    )
    for p, (a, b) in enumerate(corner_items):
        n, h, w = levels[a]
        here = pltpu.roll(corner, LANES - 8 * p, 1) if p else corner
        band(a, b)[w // LANES, pl.ds(0, SUB), :] = here
        band(a, b)[w // LANES, pl.ds(SUB + h, SUB), :] = here

    for level in range(count - 2):
        n, h, w = levels[level + 1]
        tiles = w // LANES
        low, detail, target = lows[level], details[level], lows[level + 1]

        def columns(c, carry):
            for half in range(2):
                smooth = low.at[c] if half == 0 else detail.at[0, c]
                rough = detail.at[1, c] if half == 0 else detail.at[2, c]
                out = joined.at[half, c]
                vertical(smooth, rough, out, (h + SUB) // SUB, half)
                out[pl.ds(SUB + 2 * h + LANES - SUB, SUB), :] = out[pl.ds(0, SUB), :]
            return carry

        lax.fori_loop(0, tiles + 1, columns, 0)
        smooths, roughs, spreads = (smooth_a, smooth_b), (rough_a, rough_b), (spread_a, spread_b)

        def tin(k, slot):
            turn_in(joined.at[0], smooths[slot], k, tiles)
            turn_in(joined.at[1], roughs[slot], k, tiles)

        def across(k, slot):
            horizontal(smooths[slot], roughs[slot], spreads[slot], w, True)

        def tout(k, slot):
            for j in range(2 * tiles + 1):
                target[j, block(SUB + LANES * k), :] = spreads[slot][
                    pl.ds(SUB + LANES * j, LANES), :
                ].T

        blocks_of(2 * h // LANES + 1, tin, across, tout)
        for j in range(2 * tiles + 1):
            target[j, pl.ds(0, SUB), :] = target[j, pl.ds(SUB + 2 * h + LANES - SUB, SUB), :]

    for copy in sends[early:]:
        copy.wait()
    for k in range(rest_pairs):
        unpack_rows(few_pairs + k)
    for k in range(rest_blocks):
        unpack_columns(few_blocks + k)
    n, h, w = levels[-1]
    tiles = w // LANES

    def border(c, carry):
        turn_strips(c)
        return carry

    vertical(outer.at[0, tiles], outer.at[1, tiles], tall_a, steps, 1)
    lax.fori_loop(0, tiles, border, 0)
    turn_tall(tall_a, tiles, range(last + 1))
    for k in range(last + 1):
        wrap_around(rough_out.at[k], tiles)


def finest_level(height, width, low, mixed, rough, out, joined, *refs):
    smooth_a, smooth_b, spread_a, spread_b, finished, store_sem = refs
    smooths, spreads = (smooth_a, smooth_b), (spread_a, spread_b)
    tiles = width // LANES

    def columns(c, carry):
        vertical(low.at[c], mixed.at[c], joined.at[c], (height + SUB) // SUB, 0)
        return carry

    lax.fori_loop(0, tiles + 1, columns, 0)

    def store_copy(k, j):
        rows = block(LANES * k)
        return pltpu.make_async_copy(
            finished.at[j, rows, :], out.at[rows, pl.ds(j * LANES, LANES)], store_sem.at[k, j]
        )

    def tin(k, slot):
        turn_in(joined, smooths[slot], k, tiles)

    def across(k, slot):
        horizontal(smooths[slot], rough.at[k], spreads[slot], width, False)

    def tout(k, slot):
        for j in range(2 * tiles):
            finished[j, block(LANES * k), :] = spreads[slot][pl.ds(SUB + LANES * j, LANES), :].T
            store_copy(k, j).start()

    count = 2 * height // LANES
    blocks_of(count, tin, across, tout)
    for k in range(count):
        for j in range(2 * tiles):
            store_copy(k, j).wait()


def per_device(mesh_shape, coarse, *details):
    arrays = (coarse[None],) + details
    arrays = tuple(pltpu.with_memory_space_constraint(a, pltpu.HBM) for a in arrays)
    levels = [a.shape for a in arrays]
    count = len(levels)
    f32 = jnp.float32
    vmem = lambda *dims: pltpu.VMEM(dims, f32)
    anywhere = pl.BlockSpec(memory_space=pl.ANY)
    in_vmem = pl.BlockSpec(memory_space=pltpu.VMEM)
    n_pairs = (len(row_items(levels)) + 1) // 2
    n_blocks = (len(column_blocks(levels)) + 1) // 2
    n_edges = sum(2 + len({0, w // LANES - 1}) for n, h, w in levels) + 4
    n_bodies = 3 * sum(max(w // LANES - 2, 0) for n, h, w in levels)
    n, h, w = levels[-2]
    low_shape = lambda h, w: (w // LANES + 1, SUB + h + LANES, LANES)
    detail_shape = lambda h, w: (3, w // LANES + 1, h + 2 * SUB, LANES)
    _, height, width = levels[-1]
    low, mixed, rough = pl.pallas_call(
        functools.partial(coarse_levels, mesh_shape, levels),
        out_shape=[
            vmem(*low_shape(height, width)),
            vmem(width // LANES + 1, height + 2 * SUB, LANES),
            vmem(2 * height // LANES, SUB + width + LANES, LANES),
        ],
        in_specs=[anywhere] * count,
        out_specs=[in_vmem] * 3,
        scratch_shapes=[vmem(*low_shape(h, w)) for _, h, w in levels[1:-1]]
        + [vmem(*detail_shape(h, w)) for _, h, w in levels[1:-1]]
        + [vmem(2, width // LANES + 1, height + 2 * SUB, LANES)]
        + [vmem(b, SUB, w) for b, h, w in levels] * 2
        + [vmem(2, w // LANES + 1, SUB + 2 * h + LANES, LANES)]
        + [vmem(SUB + w + LANES, LANES)] * 4
        + [vmem(SUB + 2 * w + LANES, LANES)] * 2
        + [vmem(2, 2 * STRIP, LANES)]
        + [vmem(2 * height + 2 * SUB, LANES)] * 2
        + [vmem(n_pairs, SUB, LANES)] * 4
        + [vmem(n_blocks, SUB, LANES)] * 4
        + [vmem(SUB, LANES)] * 6
        + [
            pltpu.SemaphoreType.DMA((n_edges,)),
            pltpu.SemaphoreType.DMA((max(n_bodies, 1),)),
            pltpu.SemaphoreType.DMA((12,)),
            pltpu.SemaphoreType.DMA((12,)),
        ],
        compiler_params=pltpu.CompilerParams(
            collective_id=0, has_side_effects=True, vmem_limit_bytes=40 * 1024 * 1024
        ),
        name="coarse_levels",
    )(*arrays)

    tiles = width // LANES
    return pl.pallas_call(
        functools.partial(finest_level, height, width),
        out_shape=jax.ShapeDtypeStruct((2 * height, 2 * width), f32),
        in_specs=[in_vmem] * 3,
        out_specs=anywhere,
        scratch_shapes=[vmem(tiles + 1, 2 * height + 2 * SUB, LANES)]
        + [vmem(SUB + width + LANES, LANES)] * 2
        + [vmem(2 * width + 2 * SUB, LANES)] * 2
        + [
            vmem(2 * tiles, 2 * height, LANES),
            pltpu.SemaphoreType.DMA((2 * height // LANES, 2 * tiles)),
        ],
        compiler_params=pltpu.CompilerParams(vmem_limit_bytes=40 * 1024 * 1024),
        name="finest_level",
    )(low, mixed, rough)


def solution(mesh):
    mesh_shape = (mesh.shape["rows"], mesh.shape["cols"])
    return jax.shard_map(
        functools.partial(per_device, mesh_shape),
        mesh=mesh,
        in_specs=(
            P("rows", "cols"),
            P(None, "rows", "cols"),
            P(None, "rows", "cols"),
            P(None, "rows", "cols"),
            P(None, "rows", "cols"),
        ),
        out_specs=P("rows", "cols"),
        check_vma=False,
    )
```

```python
import functools

import jax
import jax.numpy as jnp
from jax import lax
from jax.experimental import pallas as pl
from jax.experimental.pallas import tpu as pltpu
from jax.sharding import PartitionSpec as P

lift_alpha = -1.586134342059924
lift_beta = -0.052980118572961
lift_gamma = 0.882911075530934
lift_delta = 0.443506852043971
lift_scale = 1.149604398860241

MESH = pl.DeviceIdType.MESH
LANES = 128
SUB = 8
STRIP = 72
GROUP = 4
BIG, SMALL = lift_scale * lift_scale, 1.0 / (lift_scale * lift_scale)


def lanes_of(shape):
    return lax.broadcasted_iota(jnp.int32, shape, len(shape) - 1)


def rows_of(shape):
    return lax.broadcasted_iota(jnp.int32, shape, len(shape) - 2)


def eight(start):
    return pl.ds(pl.multiple_of(start, SUB), SUB)


def block(start):
    return pl.ds(pl.multiple_of(start, SUB), LANES)


def lift(get_smooth, get_rough, put_even, put_odd, steps):
    before = get_rough(-1)
    smooth = get_smooth(-1) - lift_delta * (before + get_rough(-2))
    r0 = get_rough(0)
    s1 = get_smooth(0) - lift_delta * (r0 + before)
    r2_before = before - lift_gamma * (smooth + s1)
    r0_next = get_rough(1)
    s1_next = get_smooth(1) - lift_delta * (r0_next + r0)
    r2 = r0 - lift_gamma * (s1 + s1_next)
    s3 = s1 - lift_beta * (r2 + r2_before)
    s1, r0 = s1_next, r0_next
    for v in range(steps):
        r0_next = get_rough(v + 2)
        s1_next = get_smooth(v + 2) - lift_delta * (r0_next + r0)
        r2_next = r0 - lift_gamma * (s1 + s1_next)
        s3_next = s1 - lift_beta * (r2_next + r2)
        put_even(v, s3)
        put_odd(v, r2 - lift_alpha * (s3 + s3_next))
        s1, r0, r2, s3 = s1_next, r0_next, r2_next, s3_next


def vertical(smooth_ref, rough_ref, out_ref, steps, half, first=4):
    def smooth(v):
        x = smooth_ref[pl.ds(first + v, SUB, stride=steps), :]
        return x * BIG if half == 0 else x

    def rough(v):
        x = rough_ref[pl.ds(first + v, SUB, stride=steps), :]
        return x * SMALL if half == 1 else x

    def even(v, x):
        out_ref[pl.ds(2 * v, SUB, stride=2 * steps), :] = x

    def odd(v, x):
        out_ref[pl.ds(2 * v + 1, SUB, stride=2 * steps), :] = x

    lift(smooth, rough, even, odd, steps)


def horizontal(smooth_ref, rough_ref, spread, width, wrap):
    steps = (width + SUB) // SUB

    def smooth(v):
        return smooth_ref[pl.ds(4 + v, SUB, stride=steps), :]

    def rough(v):
        return rough_ref[pl.ds(4 + v, SUB, stride=steps), :]

    def even(v, x):
        spread[pl.ds(2 * v, SUB, stride=2 * steps), :] = x

    def odd(v, x):
        spread[pl.ds(2 * v + 1, SUB, stride=2 * steps), :] = x

    lift(smooth, rough, even, odd, steps)
    if wrap:
        spread[pl.ds(SUB + 2 * width + LANES - SUB, SUB), :] = spread[pl.ds(0, SUB), :]


def turn(tall, turned, c, ks):
    for k in ks:
        turned[k, block(SUB + LANES * c), :] = tall[block(SUB + LANES * k), :].T


def wrap_around(turned, tiles):
    turned[pl.ds(0, SUB), :] = turned[pl.ds(SUB + LANES * tiles + LANES - SUB, SUB), :]


def repeat(count, body):
    if count == 1:
        body(0, 0)
    elif count:
        lax.fori_loop(0, count, body, 0)


def tiles_of(tiles, down, across):
    down(0, 0)

    def two(m, carry):
        c = 2 * m
        across(c, 0)
        down(c + 1, 1)
        across(c + 1, 1)
        down(c + 2, 0)
        return carry

    repeat(tiles // 2, two)
    if tiles % 2:
        across(tiles - 1, 0)
        down(tiles, 1)
        across(tiles, 1)
    else:
        across(tiles, 0)


def blocks_of(count, across, out):
    across(0, 0)

    def two(m, carry):
        k = 2 * m
        out(k, 0)
        across(k + 1, 1)
        out(k + 1, 1)
        across(k + 2, 0)
        return carry

    repeat((count - 1) // 2, two)
    if count % 2:
        out(count - 1, 0)
    else:
        out(count - 2, 0)
        across(count - 1, 1)
        out(count - 1, 1)


def row_split(levels):
    return (len(row_items(levels[:-1])) + 1) // 2


def column_split(levels):
    return (len(column_blocks(levels[:-1])) + 1) // 2


def row_items(levels):
    return [(a, b, c) for a, (n, h, w) in enumerate(levels) for b in range(n) for c in range(w // LANES)]


def column_blocks(levels):
    blocks, short = [], []
    for a, (n, h, w) in enumerate(levels):
        for b in range(n):
            if h < LANES:
                short.append((a, b, 0, h))
                if sum(p[3] for p in short) == LANES:
                    blocks.append(short)
                    short = []
            else:
                blocks.extend([[(a, b, LANES * k, LANES)] for k in range(h // LANES)])
    return blocks + ([short] if short else [])


def coarse_levels(mesh_shape, levels, *refs):
    count = len(levels)
    inputs, refs = refs[:count], refs[count:]
    low_out, mixed_out, rough_out, refs = refs[0], refs[1], refs[2], refs[3:]
    lows, refs = list(refs[: count - 2]) + [low_out], refs[count - 2 :]
    details, refs = refs[: count - 2], refs[count - 2 :]
    outer, refs = refs[0], refs[1:]
    tops, bottoms, refs = refs[:count], refs[count : 2 * count], refs[2 * count :]
    smooth_turned, rough_turned, strip, *refs = refs
    spreads, smooth_talls, rough_talls, refs = refs[:2], refs[2:4], refs[4:6], refs[6:]
    send_top, send_bottom, below, above, *refs = refs
    send_first, send_last, from_right, from_left, *refs = refs
    corner_top, corner_bottom, down_right, down_left, up_right, up_left, *refs = refs
    edge_sem, body_sem, send_sem, recv_sem = refs

    def band(a, b):
        if a == 0:
            return lows[0]
        if a < count - 1:
            return details[a - 1].at[b]
        return mixed_out if b == 1 else outer.at[b // 2]

    n_rows, n_cols = mesh_shape
    row, col = lax.axis_index("rows"), lax.axis_index("cols")
    row_next, row_prev = lax.rem(row + 1, n_rows), lax.rem(row + n_rows - 1, n_rows)
    col_next, col_prev = lax.rem(col + 1, n_cols), lax.rem(col + n_cols - 1, n_cols)

    barrier = pltpu.get_barrier_semaphore()
    neighbours = [
        (r, c)
        for r in (row_prev, row, row_next)
        for c in (col_prev, col, col_next)
        if not (r is row and c is col)
    ]
    for place in neighbours:
        pl.semaphore_signal(barrier, inc=1, device_id=place, device_id_type=MESH)

    edges, bodies = [], []

    def load(src, dst, sem, into):
        copy = pltpu.make_async_copy(src, dst, sem.at[len(into)])
        copy.start()
        into.append(copy)

    def load_tile(a, c, sem, into):
        n, h, w = levels[a]
        columns = pl.ds(c * LANES, LANES)
        rows = pl.ds(SUB, h)
        if a == 0:
            load(inputs[a].at[:, :, columns], lows[0].at[pl.ds(c, 1), rows, :], sem, into)
        elif a < count - 1:
            load(inputs[a].at[:, :, columns], details[a - 1].at[:, c, rows, :], sem, into)
        else:
            for b in range(n):
                load(inputs[a].at[b, :, columns], band(a, b).at[c, rows, :], sem, into)

    for a in reversed(range(count)):
        n, h, w = levels[a]
        load(inputs[a].at[:, pl.ds(0, SUB), :], tops[a], edge_sem, edges)
        load(inputs[a].at[:, pl.ds(h - SUB, SUB), :], bottoms[a], edge_sem, edges)
        for c in sorted({0, w // LANES - 1}):
            load_tile(a, c, edge_sem, edges)
    for a in range(count):
        for c in range(1, levels[a][2] // LANES - 1):
            load_tile(a, c, body_sem, bodies)

    lane = lanes_of((SUB, LANES))
    sub = rows_of((SUB, LANES))
    upper = sub < 4

    for copy in edges:
        copy.wait()

    items = row_items(levels)
    for k in range((len(items) + 1) // 2):
        pair = items[2 * k : 2 * k + 2]
        top, bottom = [
            [ref[a][b, :, pl.ds(c * LANES, LANES)] for a, b, c in pair] for ref in (tops, bottoms)
        ]
        top, bottom = [x if len(x) == 2 else x * 2 for x in (top, bottom)]
        send_top[k] = jnp.where(upper, top[0], pltpu.roll(top[1], 4, 0))
        send_bottom[k] = jnp.where(upper, pltpu.roll(bottom[1], 4, 0), bottom[0])

    corner_items = [(a, b) for a in range(count) for b in range(levels[a][0])]
    slot = lax.rem(lane + 4, LANES) // 8
    for ref, out in ((tops, corner_top), (bottoms, corner_bottom)):
        total = None
        for p, (a, b) in enumerate(corner_items):
            w = levels[a][2]
            edge = jnp.where(
                lane < 64, ref[a][b, :, pl.ds(0, LANES)], ref[a][b, :, pl.ds(w - LANES, LANES)]
            )
            if p:
                edge = pltpu.roll(edge, 8 * p, 1)
            total = edge if total is None else jnp.where(slot == p, edge, total)
        out[...] = total

    pl.semaphore_wait(barrier, len(neighbours))

    sends = []

    def send(src, dst, place):
        k = len(sends)
        copy = pltpu.make_async_remote_copy(
            src_ref=src,
            dst_ref=dst,
            send_sem=send_sem.at[k],
            recv_sem=recv_sem.at[k],
            device_id=place,
            device_id_type=MESH,
        )
        copy.start()
        sends.append(copy)

    few_pairs = row_split(levels)
    rest_pairs = (len(items) + 1) // 2 - few_pairs

    def send_rows(start, length):
        part = pl.ds(start, length)
        send(send_top.at[part], below.at[part], (row_prev, col))
        send(send_bottom.at[part], above.at[part], (row_next, col))

    send_rows(0, few_pairs)
    send(corner_top, down_right, (row_prev, col_prev))
    send(corner_top, down_left, (row_prev, col_next))
    send(corner_bottom, up_right, (row_next, col_prev))
    send(corner_bottom, up_left, (row_next, col_next))

    blocks = column_blocks(levels)
    first_half = lanes_of((LANES, LANES)) < 64
    turned = []
    for parts in blocks:
        pieces = []
        for a, b, start, length in parts:
            w = levels[a][2]
            rows = pl.ds(SUB + start, length)
            pieces.append(
                jnp.where(
                    first_half[:length],
                    band(a, b)[0, rows, :],
                    band(a, b)[w // LANES - 1, rows, :],
                )
            )
        missing = LANES - sum(p[3] for p in parts)
        if missing:
            pieces.append(jnp.zeros((missing, LANES), jnp.float32))
        whole = pieces[0] if len(pieces) == 1 else jnp.concatenate(pieces, axis=0)
        whole = whole.T
        turned.append((whole[:SUB], whole[LANES - SUB :]))
    for k in range((len(blocks) + 1) // 2):
        one = turned[2 * k]
        two = turned[min(2 * k + 1, len(blocks) - 1)]
        send_first[k] = jnp.where(upper, one[0], pltpu.roll(two[0], 4, 0))
        send_last[k] = jnp.where(upper, pltpu.roll(two[1], 4, 0), one[1])
    few_blocks = column_split(levels)
    rest_blocks = (len(blocks) + 1) // 2 - few_blocks

    def send_columns(start, length):
        part = pl.ds(start, length)
        send(send_first.at[part], from_right.at[part], (row, col_prev))
        send(send_last.at[part], from_left.at[part], (row, col_next))

    send_columns(0, few_blocks)
    early = len(sends)
    send_rows(few_pairs, rest_pairs)
    send_columns(few_blocks, rest_blocks)

    for copy in bodies:
        copy.wait()

    n, h, w = levels[-1]
    tiles = w // LANES
    steps = (h + SUB) // SUB
    last = 2 * h // LANES - 1

    inner = range(1, last)

    def down(c, slot):
        vertical(outer.at[0, c], outer.at[1, c], rough_talls[slot], steps, 1)

    down(0, 0)

    def two_tiles(m, carry):
        c = 2 * m
        turn(rough_talls[0], rough_out, c, inner)
        down(c + 1, 1)
        turn(rough_talls[1], rough_out, c + 1, inner)
        down(c + 2, 0)
        return carry

    lax.fori_loop(0, tiles // 2, two_tiles, 0)

    def unpack_rows(k):
        for i, (a, b, c) in enumerate(items[2 * k : 2 * k + 2]):
            h = levels[a][1]
            after, before = below[k], above[k]
            if i:
                after, before = pltpu.roll(after, 4, 0), pltpu.roll(before, 4, 0)
            band(a, b)[c, pl.ds(SUB + h, SUB), :] = after
            band(a, b)[c, pl.ds(0, SUB), :] = before

    def unpack_columns(k):
        for i, parts in enumerate(blocks[2 * k : 2 * k + 2]):
            after, before = from_right[k], from_left[k]
            if i:
                after, before = pltpu.roll(after, 4, 0), pltpu.roll(before, 4, 0)
            whole = jnp.concatenate(
                [after, jnp.zeros((LANES - 2 * SUB, LANES), jnp.float32), before], axis=0
            ).T
            place = 0
            for a, b, start, length in parts:
                band(a, b)[levels[a][2] // LANES, pl.ds(SUB + start, length), :] = whole[
                    place : place + length
                ]
                place += length

    for copy in sends[:early]:
        copy.wait()
    for k in range(few_pairs):
        unpack_rows(k)
    for k in range(few_blocks):
        unpack_columns(k)
    right_side = lax.rem(lane, 8) < 4
    corner = jnp.where(
        upper,
        jnp.where(right_side, down_right[...], down_left[...]),
        jnp.where(right_side, up_right[...], up_left[...]),
    )
    for p, (a, b) in enumerate(corner_items):
        n, h, w = levels[a]
        here = pltpu.roll(corner, LANES - 8 * p, 1) if p else corner
        band(a, b)[w // LANES, pl.ds(0, SUB), :] = here
        band(a, b)[w // LANES, pl.ds(SUB + h, SUB), :] = here

    for level in range(count - 2):
        n, h, w = levels[level + 1]
        tiles = w // LANES
        low, detail, target = lows[level], details[level], lows[level + 1]

        count_k = 2 * h // LANES + 1

        def down(c, slot):
            for half, tall in enumerate((smooth_talls[slot], rough_talls[slot])):
                smooth = low.at[c] if half == 0 else detail.at[0, c]
                rough = detail.at[1, c] if half == 0 else detail.at[2, c]
                vertical(smooth, rough, tall, (h + SUB) // SUB, half)
                tall[pl.ds(SUB + 2 * h + LANES - SUB, SUB), :] = tall[pl.ds(0, SUB), :]

        def across(c, slot):
            turn(smooth_talls[slot], smooth_turned, c, range(count_k))
            turn(rough_talls[slot], rough_turned, c, range(count_k))

        tiles_of(tiles, down, across)
        for k in range(count_k):
            wrap_around(smooth_turned.at[k], tiles)
            wrap_around(rough_turned.at[k], tiles)

        def lift_columns(k, slot):
            horizontal(smooth_turned.at[k], rough_turned.at[k], spreads[slot], w, True)

        def tout(k, slot):
            for j in range(2 * tiles + 1):
                target[j, block(SUB + LANES * k), :] = spreads[slot][
                    pl.ds(SUB + LANES * j, LANES), :
                ].T

        blocks_of(count_k, lift_columns, tout)
        for j in range(2 * tiles + 1):
            target[j, pl.ds(0, SUB), :] = target[j, pl.ds(SUB + 2 * h + LANES - SUB, SUB), :]

    for copy in sends[early:]:
        copy.wait()
    for k in range(rest_pairs):
        unpack_rows(few_pairs + k)
    for k in range(rest_blocks):
        unpack_columns(few_blocks + k)
    n, h, w = levels[-1]
    tiles = w // LANES

    vertical(outer.at[0, tiles], outer.at[1, tiles], rough_talls[0], steps, 1)
    turn(rough_talls[0], rough_out, tiles, range(last + 1))

    def border(m, carry):
        for u in range(GROUP):
            c = GROUP * m + u
            for i, first in enumerate((4, 4 + h + SUB - STRIP)):
                vertical(outer.at[0, c], outer.at[1, c], strip.at[u, i], STRIP // SUB, 1, first)
        for u in range(GROUP):
            c = GROUP * m + u
            for i, k in enumerate((0, last)):
                rough_out[k, block(SUB + LANES * c), :] = strip[u, i, pl.ds(SUB, LANES), :].T
        return carry

    repeat(tiles // GROUP, border)
    for k in range(last + 1):
        wrap_around(rough_out.at[k], tiles)


def finest_level(height, width, low, mixed, rough, out, *refs):
    tall_a, tall_b, turned, spread_a, spread_b, finished, store_sem = refs
    talls, spreads = (tall_a, tall_b), (spread_a, spread_b)
    tiles = width // LANES
    count = 2 * height // LANES

    def down(c, slot):
        vertical(low.at[c], mixed.at[c], talls[slot], (height + SUB) // SUB, 0)

    def across(c, slot):
        turn(talls[slot], turned, c, range(count))

    tiles_of(tiles, down, across)
    for k in range(count):
        wrap_around(turned.at[k], tiles)

    def store_copy(k):
        rows = block(LANES * k)
        return pltpu.make_async_copy(finished.at[rows, :], out.at[rows, :], store_sem.at[k])

    def lift_columns(k, slot):
        horizontal(turned.at[k], rough.at[k], spreads[slot], width, False)

    def tout(k, slot):
        for j in range(2 * tiles):
            finished[block(LANES * k), pl.ds(LANES * j, LANES)] = spreads[slot][
                pl.ds(SUB + LANES * j, LANES), :
            ].T
        store_copy(k).start()

    blocks_of(count, lift_columns, tout)
    for k in range(count):
        store_copy(k).wait()


def per_device(mesh_shape, coarse, *details):
    arrays = (coarse[None],) + details
    arrays = tuple(pltpu.with_memory_space_constraint(a, pltpu.HBM) for a in arrays)
    levels = [a.shape for a in arrays]
    count = len(levels)
    f32 = jnp.float32
    vmem = lambda *dims: pltpu.VMEM(dims, f32)
    anywhere = pl.BlockSpec(memory_space=pl.ANY)
    in_vmem = pl.BlockSpec(memory_space=pltpu.VMEM)
    n_pairs = (len(row_items(levels)) + 1) // 2
    n_blocks = (len(column_blocks(levels)) + 1) // 2
    n_edges = sum(2 + len({0, w // LANES - 1}) for n, h, w in levels) + 4
    n_bodies = 3 * sum(max(w // LANES - 2, 0) for n, h, w in levels)
    n, h, w = levels[-2]
    low_shape = lambda h, w: (w // LANES + 1, SUB + h + LANES, LANES)
    detail_shape = lambda h, w: (3, w // LANES + 1, h + 2 * SUB, LANES)
    _, height, width = levels[-1]
    low, mixed, rough = pl.pallas_call(
        functools.partial(coarse_levels, mesh_shape, levels),
        out_shape=[
            vmem(*low_shape(height, width)),
            vmem(width // LANES + 1, height + 2 * SUB, LANES),
            vmem(2 * height // LANES, SUB + width + LANES, LANES),
        ],
        in_specs=[anywhere] * count,
        out_specs=[in_vmem] * 3,
        scratch_shapes=[vmem(*low_shape(h, w)) for _, h, w in levels[1:-1]]
        + [vmem(*detail_shape(h, w)) for _, h, w in levels[1:-1]]
        + [vmem(2, width // LANES + 1, height + 2 * SUB, LANES)]
        + [vmem(b, SUB, w) for b, h, w in levels] * 2
        + [vmem(2 * h // LANES + 1, SUB + w + LANES, LANES)] * 2
        + [vmem(GROUP, 2, 2 * STRIP, LANES)]
        + [vmem(SUB + 2 * w + LANES, LANES)] * 2
        + [vmem(2 * height + 2 * SUB, LANES)] * 4
        + [vmem(n_pairs, SUB, LANES)] * 4
        + [vmem(n_blocks, SUB, LANES)] * 4
        + [vmem(SUB, LANES)] * 6
        + [
            pltpu.SemaphoreType.DMA((n_edges,)),
            pltpu.SemaphoreType.DMA((max(n_bodies, 1),)),
            pltpu.SemaphoreType.DMA((12,)),
            pltpu.SemaphoreType.DMA((12,)),
        ],
        compiler_params=pltpu.CompilerParams(
            collective_id=0, has_side_effects=True, vmem_limit_bytes=40 * 1024 * 1024
        ),
        name="coarse_levels",
    )(*arrays)

    tiles = width // LANES
    return pl.pallas_call(
        functools.partial(finest_level, height, width),
        out_shape=jax.ShapeDtypeStruct((2 * height, 2 * width), f32),
        in_specs=[in_vmem] * 3,
        out_specs=anywhere,
        scratch_shapes=[vmem(2 * height + 2 * SUB, LANES)] * 2
        + [vmem(2 * height // LANES, SUB + width + LANES, LANES)]
        + [vmem(2 * width + 2 * SUB, LANES)] * 2
        + [
            vmem(2 * height, 2 * width),
            pltpu.SemaphoreType.DMA((2 * height // LANES,)),
        ],
        compiler_params=pltpu.CompilerParams(vmem_limit_bytes=40 * 1024 * 1024),
        name="finest_level",
    )(low, mixed, rough)


def solution(mesh):
    mesh_shape = (mesh.shape["rows"], mesh.shape["cols"])
    return jax.shard_map(
        functools.partial(per_device, mesh_shape),
        mesh=mesh,
        in_specs=(
            P("rows", "cols"),
            P(None, "rows", "cols"),
            P(None, "rows", "cols"),
            P(None, "rows", "cols"),
            P(None, "rows", "cols"),
        ),
        out_specs=P("rows", "cols"),
        check_vma=False,
    )
```
